32 devices in a mesh: grp: 4 (over x, core), lat: 8 (over z, y).
Axes of the slice: x: 2, y: 2, z: 4, core: 2. Of those that a mesh axis runs over, the one named last changes fastest.
Arguments:
- grid_state: bfloat16 [16, 192, 384, 128], P('grp', 'lat'), may hold values from -6 to 6
- noise_field: bfloat16 [16, 192, 384, 128], P('grp', 'lat'), may hold values from -6 to 6
- legendre: bfloat16 [192, 128, 128], P('lat'), may hold values from -0.4375 to 0.4375
- diffusion: float32 [128], replicated, may hold values from 0.1 to 10
- input_weight: bfloat16 [128, 256], replicated, may hold values from -0.5 to 0.5
- noise_weight: bfloat16 [128, 256], replicated, may hold values from -0.5 to 0.5
- input_bias: float32 [256], replicated, may hold values from -4 to 4
- middle_weight: bfloat16 [256, 256], replicated, may hold values from -0.375 to 0.375
- output_weight: bfloat16 [256, 128], replicated, may hold values from -0.375 to 0.375
Outputs:
- new_state: bfloat16 [16, 192, 384, 128], P('grp', 'lat')
- ens_mean: float32 [192, 384, 128], P('lat')
- ens_var: float32 [192, 384, 128], P('lat')
The draws below stay inside these ranges and needn't reach their ends.
All inputs are finite; a program needn't handle non-finite values.
Results may differ from the reference program's by a relative error of at most 0.012.
Values may be sent and summed in bfloat16 or wider, within the bound.
A program may use at most 192 MiB of HBM per device.

```python
import math
import jax
import jax.numpy as jnp
from jax import lax

CHAN = 128
NLON = 384
NLAT = 192
WAVES = 128
NOISE = 128
HIDDEN_SIZE = 256
MEMBERS = 16


def levels(key, extent, shards, low, largest):
    loudness = 1.0
    for dim, blocks in shards:
        draws = jax.random.uniform(jax.random.fold_in(jax.random.fold_in(key, 6), dim), (blocks,), jnp.float32, low / len(shards), largest / len(shards))
        loudness = loudness * jnp.repeat(jnp.exp(draws), extent[dim] // blocks).reshape((-1,) + (1,) * (len(extent) - 1 - dim))
    return loudness


def gaussian(own_key, shape, deviation, most, pieces=(), held_as=jnp.bfloat16):
    result = jax.random.normal(own_key, shape, jnp.float32) * deviation
    if len(pieces) > 0:
        result = levels(own_key, shape, pieces, -0.22, 0.18) * result
    return jnp.clip(result, min=-most, max=most).astype(held_as)


def setup_inputs(seed: int = 0) -> dict:
    arg_keys = jax.random.split(jax.random.key(seed), 10)
    grid_state = gaussian(arg_keys[0], (MEMBERS, NLAT, NLON, CHAN), 1.0, 6.0, ((0, 4), (1, 8)))
    noise_field = gaussian(arg_keys[1], (MEMBERS, NLAT, NLON, NOISE), 1.0, 6.0, ((0, 4), (1, 8)))
    legendre = gaussian(arg_keys[2], (NLAT, WAVES, WAVES), NLAT ** -0.5, 0.4375, ((0, 8),))
    diffusion = jnp.clip(jnp.exp(jax.random.uniform(arg_keys[3], (CHAN,), jnp.float32, math.log(0.1), math.log(10.0))), 0.1, 10.0)
    input_weight = gaussian(arg_keys[4], (CHAN, HIDDEN_SIZE), CHAN ** -0.5, 0.5)
    noise_weight = gaussian(arg_keys[5], (NOISE, HIDDEN_SIZE), NOISE ** -0.5, 0.5)
    input_bias = gaussian(arg_keys[6], (HIDDEN_SIZE,), 1.0, 4.0, (), jnp.float32)
    middle_weight = gaussian(arg_keys[7], (HIDDEN_SIZE, HIDDEN_SIZE), HIDDEN_SIZE ** -0.5, 0.375)
    output_weight = gaussian(arg_keys[8], (HIDDEN_SIZE, CHAN), HIDDEN_SIZE ** -0.5, 0.375)
    return {"grid_state": grid_state, "noise_field": noise_field, "legendre": legendre, "diffusion": diffusion, "input_weight": input_weight, "noise_weight": noise_weight, "input_bias": input_bias, "middle_weight": middle_weight, "output_weight": output_weight}


def wave_table(lon_count, wave_count):
    lon_ids = jnp.arange(lon_count, dtype=jnp.int32)[:, None]
    wave_ids = jnp.arange(wave_count, dtype=jnp.int32)[None, :]
    phase = (lon_ids * wave_ids % lon_count).astype(jnp.float32) * (2.0 * math.pi / lon_count)
    factor = math.sqrt(2.0 / lon_count)
    joined = jnp.concatenate([jnp.cos(phase), -jnp.sin(phase)], axis=1) * factor
    return joined.astype(jnp.bfloat16)

def damping_filter(diffusion, wave_count):
    degree = jnp.arange(wave_count, dtype=jnp.int32).astype(jnp.float32)
    ratio = degree * (degree + 1.0) / float((wave_count - 1) * wave_count)
    return 1.0 / (1.0 + diffusion[None, :] * (ratio * ratio)[:, None])

def reference(grid_state, noise_field, legendre, diffusion, input_weight, noise_weight, input_bias, middle_weight, output_weight):
    transform = wave_table(NLON, WAVES).astype(jnp.float32)
    legendre_values = legendre.astype(jnp.float32)
    wave_ids = jnp.arange(WAVES, dtype=jnp.int32)
    triangle = (wave_ids[None, :] >= wave_ids[:, None]).astype(jnp.float32)
    damping = damping_filter(diffusion, WAVES)

    def advance(pair):
        member_state, member_noise = pair
        fourier = jnp.einsum('lxc,xk->lkc', member_state.astype(jnp.float32), transform).astype(jnp.bfloat16)
        fourier = fourier.reshape(NLAT, 2, WAVES, CHAN).astype(jnp.float32)
        spectrum = jnp.einsum('lmn,lrmc->rmnc', legendre_values, fourier) * triangle[None, :, :, None]
        filtered = (spectrum * damping[None, None, :, :]).astype(jnp.bfloat16)
        grid_fourier = jnp.einsum('lmn,rmnc->lrmc', legendre_values, filtered.astype(jnp.float32)).astype(jnp.bfloat16)
        grid_fourier = grid_fourier.reshape(NLAT, 2 * WAVES, CHAN).astype(jnp.float32)
        smoothed = jnp.einsum('lkc,xk->lxc', grid_fourier, transform)
        flat_fields = smoothed.reshape(-1, CHAN)
        smoothed_in = flat_fields.astype(jnp.bfloat16)
        pre_act = jnp.dot(smoothed_in, input_weight, preferred_element_type=jnp.float32)
        pre_act = pre_act + jnp.dot(member_noise.reshape(-1, NOISE), noise_weight, preferred_element_type=jnp.float32)
        hidden_one = jax.nn.silu(pre_act + input_bias).astype(jnp.bfloat16)
        hidden_two = jax.nn.silu(jnp.dot(hidden_one, middle_weight, preferred_element_type=jnp.float32)).astype(jnp.bfloat16)
        tendency = jnp.dot(hidden_two, output_weight, preferred_element_type=jnp.float32)
        return (flat_fields + tendency).astype(jnp.bfloat16).reshape(NLAT, NLON, CHAN)
    new_state = lax.map(advance, (grid_state, noise_field))
    member_values = new_state.astype(jnp.float32)
    ens_mean = lax.optimization_barrier(jnp.mean(member_values, axis=0))
    ens_var = lax.optimization_barrier(jnp.sum(jnp.square(member_values - ens_mean), axis=0)) / (MEMBERS - 1)
    return (new_state, ens_mean, ens_var)
```

```python
import functools
import math

import jax
import jax.numpy as jnp
from jax import lax
from jax.experimental import pallas as pl
from jax.experimental.pallas import tpu as pltpu
from jax.sharding import PartitionSpec as P

BF16 = jnp.bfloat16
F32 = jnp.float32


def wave_table(lon_count, wave_count):
    lon_ids = jnp.arange(lon_count, dtype=jnp.int32)[:, None]
    wave_ids = jnp.arange(wave_count, dtype=jnp.int32)[None, :]
    phase = (lon_ids * wave_ids % lon_count).astype(jnp.float32) * (2.0 * math.pi / lon_count)
    factor = math.sqrt(2.0 / lon_count)
    joined = jnp.concatenate([jnp.cos(phase), -jnp.sin(phase)], axis=1) * factor
    return joined.astype(jnp.bfloat16)


def damping_filter(diffusion, wave_count):
    degree = jnp.arange(wave_count, dtype=jnp.int32).astype(jnp.float32)
    ratio = degree * (degree + 1.0) / float((wave_count - 1) * wave_count)
    return 1.0 / (1.0 + diffusion[None, :] * (ratio * ratio)[:, None])


def analysis_body(table_ref, grid_ref, out_ref):
    bands, _, rows, width, channels = out_ref.shape
    for row in range(0, rows, 2):
        pair = jnp.concatenate([grid_ref[0, row], grid_ref[0, row + 1]], axis=1)
        waves = jnp.dot(table_ref[...], pair, preferred_element_type=F32).astype(BF16)
        for k in range(2):
            out_ref[:, 0, row + k] = waves[:, k * channels:(k + 1) * channels].reshape(
                bands, width, channels
            )


def analyse(grid_state, table, first, count, bands):
    _, lat_rows, lon_count, channels = grid_state.shape
    width = table.shape[0] // bands
    rows = 6
    return pl.pallas_call(
        analysis_body,
        grid=(count, lat_rows // rows),
        in_specs=[
            pl.BlockSpec(table.shape, lambda b, i: (0, 0)),
            pl.BlockSpec((1, rows, lon_count, channels), lambda b, i: (b + first, i, 0, 0)),
        ],
        out_specs=pl.BlockSpec((bands, 1, rows, width, channels), lambda b, i: (0, b, i, 0, 0)),
        out_shape=jax.ShapeDtypeStruct((bands, count, lat_rows, width, channels), BF16),
        cost_estimate=pl.CostEstimate(
            flops=2 * count * lat_rows * lon_count * channels * table.shape[0],
            bytes_accessed=4 * count * lat_rows * lon_count * channels,
            transcendentals=0,
        ),
    )(table, grid_state)


def spectral_body(parts, in_ref, basis_ref, flipped_ref, damping_ref, *rest):
    outs, (fin, fout) = rest[:parts], rest[parts:]
    bands, _, lat_rows, width, channels = in_ref.shape
    waves = basis_ref.shape[0]
    lats = bands * lat_rows
    span = lat_rows * width
    for s in range(bands):
        fin[pl.ds(s * span, span), :] = in_ref[s, 0].astype(F32).reshape(span, channels)
    damping = jnp.concatenate([damping_ref[...]] * 2, axis=1)
    for m in range(waves):
        values = jnp.concatenate(
            [fin[pl.ds(r * waves + m, lats, stride=width), :] for r in range(2)], axis=1
        ).astype(BF16)
        spectrum = jnp.dot(flipped_ref[m], values, preferred_element_type=F32)
        filtered = (spectrum * damping).astype(BF16)
        grid = jnp.dot(basis_ref[m], filtered, preferred_element_type=F32)
        for r in range(2):
            fout[pl.ds(r * waves + m, lats, stride=width), :] = grid[
                :, r * channels:(r + 1) * channels
            ]
    part_rows = lat_rows // parts
    for q in range(parts):
        for s in range(bands):
            start = (s * lat_rows + q * part_rows) * width
            outs[q][s, 0] = (
                fout[pl.ds(start, part_rows * width), :]
                .reshape(part_rows, width, channels)
                .astype(BF16)
            )


def spectral(received, basis, flipped, damping, parts):
    bands, count, lat_rows, width, channels = received.shape
    part_rows = lat_rows // parts
    whole = lambda a: pl.BlockSpec(a.shape, lambda b: (0,) * a.ndim)
    return pl.pallas_call(
        functools.partial(spectral_body, parts),
        grid=(count,),
        in_specs=[
            pl.BlockSpec((bands, 1, lat_rows, width, channels), lambda b: (0, b, 0, 0, 0)),
            whole(basis),
            whole(flipped),
            whole(damping),
        ],
        out_specs=[
            pl.BlockSpec((bands, 1, part_rows, width, channels), lambda b: (0, b, 0, 0, 0))
        ] * parts,
        out_shape=[
            jax.ShapeDtypeStruct((bands, count, part_rows, width, channels), BF16)
        ] * parts,
        scratch_shapes=[pltpu.VMEM((bands * lat_rows * width, channels), F32)] * 2,
        cost_estimate=pl.CostEstimate(
            flops=8 * count * basis.size * channels,
            bytes_accessed=4 * received.size,
            transcendentals=0,
        ),
    )(received, basis, flipped, damping)


def silu(value):
    half = 0.5 * value
    return half + half * jnp.tanh(half)


def physics_body(groups, *refs):
    fields = refs[:groups]
    noise_ref, table_ref, first_ref, bias_ref, middle_ref, last_ref = refs[groups:groups + 6]
    state_ref, stats_ref = refs[-2:]
    members, _, lon_count, channels = noise_ref.shape
    states = []
    for ref in fields:
        count = ref.shape[1]
        waves = jnp.concatenate(
            [ref[:, k, 0].reshape(-1, channels) for k in range(count)], axis=1
        )
        smoothed = jnp.dot(table_ref[...], waves, preferred_element_type=F32)
        for k in range(count):
            flat = smoothed[:, k * channels:(k + 1) * channels]
            b = len(states)
            joined = jnp.concatenate([flat.astype(BF16), noise_ref[b, 0]], axis=1)
            pre = jnp.dot(joined, first_ref[...], preferred_element_type=F32)
            one = silu(pre + bias_ref[...]).astype(BF16)
            two = silu(jnp.dot(one, middle_ref[...], preferred_element_type=F32)).astype(BF16)
            tendency = jnp.dot(two, last_ref[...], preferred_element_type=F32)
            state = (flat + tendency).astype(BF16)
            state_ref[b, 0] = state
            states.append(state)
    values = [s.astype(F32) for s in states]
    total = functools.reduce(jnp.add, values)
    mean = total * (1.0 / members)
    spread = functools.reduce(jnp.add, [jnp.square(v - mean) for v in values])
    half = lon_count // 2
    for h in range(2):
        stats_ref[h, 0, 0] = total[h * half:(h + 1) * half].astype(BF16)
        stats_ref[h, 1, 0] = spread[h * half:(h + 1) * half].astype(BF16)


def physics(fields, noise, table, first, bias, middle, last, part, previous):
    bands, _, part_rows, width, channels = fields[0].shape
    members, lat_rows, lon_count, noise_channels = noise.shape
    whole = lambda a: pl.BlockSpec(a.shape, lambda i: (0,) * a.ndim)
    at = part * part_rows
    specs = [
        pl.BlockSpec((bands, f.shape[1], 1, width, channels), lambda i: (0, 0, i, 0, 0))
        for f in fields
    ]
    specs.append(
        pl.BlockSpec((members, 1, lon_count, noise_channels), lambda i: (0, i + at, 0, 0))
    )
    params = [table, first, bias, middle, last]
    specs += [whole(a) for a in params]
    operands = [*fields, noise, *params]
    aliases = {}
    if previous is not None:
        aliases = {len(operands): 0}
        operands.append(previous)
        specs.append(pl.BlockSpec(memory_space=pl.ANY))
    columns = members * part_rows * lon_count
    hidden = middle.shape[0]
    return pl.pallas_call(
        functools.partial(physics_body, len(fields)),
        grid=(part_rows,),
        in_specs=specs,
        out_specs=[
            pl.BlockSpec((members, 1, lon_count, channels), lambda i: (0, i + at, 0, 0)),
            pl.BlockSpec((2, 2, 1, lon_count // 2, channels), lambda i: (0, 0, i, 0, 0)),
        ],
        out_shape=[
            jax.ShapeDtypeStruct((members, lat_rows, lon_count, channels), BF16),
            jax.ShapeDtypeStruct((2, 2, part_rows, lon_count // 2, channels), BF16),
        ],
        input_output_aliases=aliases,
        cost_estimate=pl.CostEstimate(
            flops=2 * columns * (first.size + middle.size + last.size + 256 * channels),
            bytes_accessed=8 * columns * channels,
            transcendentals=2 * columns * hidden,
        ),
    )(*operands)


def ensemble_moments(stats, members):
    groups = lax.axis_size("grp")
    core = lax.axis_index("grp") % 2

    def swap(value, bit):
        return lax.ppermute(value, "grp", [(g, g ^ bit) for g in range(groups)])

    def join(a, b, count):
        a, b = a.astype(F32), b.astype(F32)
        total = a[0] + b[0]
        spread = (a[1] + b[1]) + jnp.square(a[0] - b[0]) * (0.5 / count)
        return jnp.stack([total, spread])

    own = lax.dynamic_index_in_dim(stats, core, 0, keepdims=False)
    other = lax.dynamic_index_in_dim(stats, 1 - core, 0, keepdims=False)
    held = join(own, swap(other, 1), members)
    bit, count = 2, 2 * members
    while bit < groups:
        held = held.astype(BF16)
        held = join(held, swap(held, bit), count)
        bit, count = 2 * bit, 2 * count
    scale = jnp.array([1.0 / count, 1.0 / (count - 1)], F32)
    held = (held * scale[:, None, None, None]).astype(BF16)
    partner = swap(held, 1)
    low = jnp.where(core == 0, held, partner)
    high = jnp.where(core == 0, partner, held)
    return low, high


def per_device(
    grid_state,
    noise_field,
    legendre,
    diffusion,
    input_weight,
    noise_weight,
    input_bias,
    middle_weight,
    output_weight,
):
    members, lat_rows, lon_count, channels = grid_state.shape
    wave_count = legendre.shape[1]
    bands = lax.axis_size("lat")
    local_waves = wave_count // bands
    chunk = 2
    parts = 2
    transform = wave_table(lon_count, wave_count)
    table = (
        transform.reshape(lon_count, 2, bands, local_waves)
        .transpose(0, 2, 1, 3)
        .reshape(lon_count, 2 * wave_count)
    )
    table_t = table.T
    exchange = lambda v: lax.all_to_all(v, "lat", split_axis=0, concat_axis=0, tiled=True)
    damping = damping_filter(diffusion, wave_count)

    sent = [
        analyse(grid_state, table_t, b, chunk, bands) for b in range(0, members, chunk)
    ]
    basis = lax.all_to_all(legendre, "lat", split_axis=1, concat_axis=0, tiled=True)
    zonal_ids = lax.axis_index("lat") * local_waves + jnp.arange(local_waves, dtype=jnp.int32)
    total_ids = jnp.arange(wave_count, dtype=jnp.int32)
    triangle = total_ids[None, :] >= zonal_ids[:, None]
    basis = jnp.where(triangle[None], basis, jnp.zeros_like(basis)).transpose(1, 0, 2)
    flipped = basis.transpose(0, 2, 1)
    received = [exchange(s) for s in sent]
    banded = [spectral(r, basis, flipped, damping, parts) for r in received]

    first = jnp.concatenate([input_weight, noise_weight], axis=0)
    new_state = None
    moments = []
    for q in range(parts):
        fields = [exchange(g[q]) for g in banded]
        new_state, stats = physics(
            fields, noise_field, table, first, input_bias[None], middle_weight,
            output_weight, q, new_state,
        )
        moments.append(ensemble_moments(stats, members))
    joined = [jnp.concatenate([low, high], axis=2) for low, high in moments]
    ens_mean = jnp.concatenate([j[0] for j in joined], axis=0).astype(F32)
    ens_var = jnp.concatenate([j[1] for j in joined], axis=0).astype(F32)
    return (new_state, ens_mean, ens_var)


def solution(mesh):
    in_specs = (
        P("grp", "lat", None, None),
        P("grp", "lat", None, None),
        P("lat", None, None),
        P(),
        P(),
        P(),
        P(),
        P(),
        P(),
    )
    out_specs = (P("grp", "lat", None, None), P("lat", None, None), P("lat", None, None))
    return jax.shard_map(
        per_device, mesh=mesh, in_specs=in_specs, out_specs=out_specs, check_vma=False
    )
```

```python
import functools
import math

import jax
import jax.numpy as jnp
from jax import lax
from jax.experimental import pallas as pl
from jax.experimental.pallas import tpu as pltpu
from jax.sharding import PartitionSpec as P

BF16 = jnp.bfloat16
F32 = jnp.float32


def wave_table(lon_count, wave_count):
    lon_ids = jnp.arange(lon_count, dtype=jnp.int32)[:, None]
    wave_ids = jnp.arange(wave_count, dtype=jnp.int32)[None, :]
    phase = (lon_ids * wave_ids % lon_count).astype(jnp.float32) * (2.0 * math.pi / lon_count)
    factor = math.sqrt(2.0 / lon_count)
    joined = jnp.concatenate([jnp.cos(phase), -jnp.sin(phase)], axis=1) * factor
    return joined.astype(jnp.bfloat16)


def damping_filter(diffusion, wave_count):
    degree = jnp.arange(wave_count, dtype=jnp.int32).astype(jnp.float32)
    ratio = degree * (degree + 1.0) / float((wave_count - 1) * wave_count)
    return 1.0 / (1.0 + diffusion[None, :] * (ratio * ratio)[:, None])


def analysis_body(table_ref, grid_ref, out_ref):
    bands, _, rows, width, channels = out_ref.shape
    for row in range(0, rows, 2):
        pair = jnp.concatenate([grid_ref[0, row], grid_ref[0, row + 1]], axis=1)
        waves = jnp.dot(table_ref[...], pair, preferred_element_type=F32).astype(BF16)
        for k in range(2):
            out_ref[:, 0, row + k] = waves[:, k * channels:(k + 1) * channels].reshape(
                bands, width, channels
            )


def analyse(grid_state, table, first, count, bands):
    _, lat_rows, lon_count, channels = grid_state.shape
    width = table.shape[0] // bands
    rows = 6
    return pl.pallas_call(
        analysis_body,
        grid=(count, lat_rows // rows),
        in_specs=[
            pl.BlockSpec(table.shape, lambda b, i: (0, 0)),
            pl.BlockSpec((1, rows, lon_count, channels), lambda b, i: (b + first, i, 0, 0)),
        ],
        out_specs=pl.BlockSpec((bands, 1, rows, width, channels), lambda b, i: (0, b, i, 0, 0)),
        out_shape=jax.ShapeDtypeStruct((bands, count, lat_rows, width, channels), BF16),
        cost_estimate=pl.CostEstimate(
            flops=2 * count * lat_rows * lon_count * channels * table.shape[0],
            bytes_accessed=4 * count * lat_rows * lon_count * channels,
            transcendentals=0,
        ),
    )(table, grid_state)


def spectral_body(parts, in_ref, basis_ref, flipped_ref, damping_ref, *rest):
    outs, (fin, fout) = rest[:parts], rest[parts:]
    bands, _, lat_rows, width, channels = in_ref.shape
    waves = basis_ref.shape[0]
    lats = bands * lat_rows
    span = lat_rows * width
    for s in range(bands):
        fin[pl.ds(s * span, span), :] = in_ref[s, 0].astype(F32).reshape(span, channels)
    damping = jnp.concatenate([damping_ref[...]] * 2, axis=1)
    for m in range(waves):
        values = jnp.concatenate(
            [fin[pl.ds(r * waves + m, lats, stride=width), :] for r in range(2)], axis=1
        ).astype(BF16)
        spectrum = jnp.dot(flipped_ref[m], values, preferred_element_type=F32)
        filtered = (spectrum * damping).astype(BF16)
        grid = jnp.dot(basis_ref[m], filtered, preferred_element_type=F32)
        for r in range(2):
            fout[pl.ds(r * waves + m, lats, stride=width), :] = grid[
                :, r * channels:(r + 1) * channels
            ]
    part_rows = lat_rows // parts
    for q in range(parts):
        for s in range(bands):
            start = (s * lat_rows + q * part_rows) * width
            outs[q][s, 0] = (
                fout[pl.ds(start, part_rows * width), :]
                .reshape(part_rows, width, channels)
                .astype(BF16)
            )


def spectral(received, basis, flipped, damping, parts):
    bands, count, lat_rows, width, channels = received.shape
    part_rows = lat_rows // parts
    whole = lambda a: pl.BlockSpec(a.shape, lambda b: (0,) * a.ndim)
    return pl.pallas_call(
        functools.partial(spectral_body, parts),
        grid=(count,),
        in_specs=[
            pl.BlockSpec((bands, 1, lat_rows, width, channels), lambda b: (0, b, 0, 0, 0)),
            whole(basis),
            whole(flipped),
            whole(damping),
        ],
        out_specs=[
            pl.BlockSpec((bands, 1, part_rows, width, channels), lambda b: (0, b, 0, 0, 0))
        ] * parts,
        out_shape=[
            jax.ShapeDtypeStruct((bands, count, part_rows, width, channels), BF16)
        ] * parts,
        scratch_shapes=[pltpu.VMEM((bands * lat_rows * width, channels), F32)] * 2,
        cost_estimate=pl.CostEstimate(
            flops=8 * count * basis.size * channels,
            bytes_accessed=4 * received.size,
            transcendentals=0,
        ),
    )(received, basis, flipped, damping)


def silu(value):
    half = 0.5 * value
    return half + half * jnp.tanh(half)


def physics_body(groups, *refs):
    fields = refs[:groups]
    noise_ref, table_ref, first_ref, bias_ref, middle_ref, last_ref = refs[groups:groups + 6]
    state_ref, stats_ref = refs[-2:]
    members, _, lon_count, channels = noise_ref.shape
    states = []
    for ref in fields:
        count = ref.shape[1]
        waves = jnp.concatenate(
            [ref[:, k, 0].reshape(-1, channels) for k in range(count)], axis=1
        )
        smoothed = jnp.dot(table_ref[...], waves, preferred_element_type=F32)
        for k in range(count):
            flat = smoothed[:, k * channels:(k + 1) * channels]
            b = len(states)
            joined = jnp.concatenate([flat.astype(BF16), noise_ref[b, 0]], axis=1)
            pre = jnp.dot(joined, first_ref[...], preferred_element_type=F32)
            one = silu(pre + bias_ref[...]).astype(BF16)
            two = silu(jnp.dot(one, middle_ref[...], preferred_element_type=F32)).astype(BF16)
            tendency = jnp.dot(two, last_ref[...], preferred_element_type=F32)
            state = (flat + tendency).astype(BF16)
            state_ref[b, 0] = state
            states.append(state)
    values = [s.astype(F32) for s in states]
    total = functools.reduce(jnp.add, values)
    mean = total * (1.0 / members)
    spread = functools.reduce(jnp.add, [jnp.square(v - mean) for v in values])
    half = lon_count // 2
    for h in range(2):
        stats_ref[h, 0, 0] = total[h * half:(h + 1) * half].astype(BF16)
        stats_ref[h, 1, 0] = spread[h * half:(h + 1) * half].astype(BF16)


def physics(fields, noise, table, first, bias, middle, last, part, previous):
    bands, _, part_rows, width, channels = fields[0].shape
    members, lat_rows, lon_count, noise_channels = noise.shape
    whole = lambda a: pl.BlockSpec(a.shape, lambda i: (0,) * a.ndim)
    at = part * part_rows
    specs = [
        pl.BlockSpec((bands, f.shape[1], 1, width, channels), lambda i: (0, 0, i, 0, 0))
        for f in fields
    ]
    specs.append(
        pl.BlockSpec((members, 1, lon_count, noise_channels), lambda i: (0, i + at, 0, 0))
    )
    params = [table, first, bias, middle, last]
    specs += [whole(a) for a in params]
    operands = [*fields, noise, *params]
    aliases = {}
    if previous is not None:
        aliases = {len(operands): 0}
        operands.append(previous)
        specs.append(pl.BlockSpec(memory_space=pl.ANY))
    columns = members * part_rows * lon_count
    hidden = middle.shape[0]
    return pl.pallas_call(
        functools.partial(physics_body, len(fields)),
        grid=(part_rows,),
        in_specs=specs,
        out_specs=[
            pl.BlockSpec((members, 1, lon_count, channels), lambda i: (0, i + at, 0, 0)),
            pl.BlockSpec((2, 2, 1, lon_count // 2, channels), lambda i: (0, 0, i, 0, 0)),
        ],
        out_shape=[
            jax.ShapeDtypeStruct((members, lat_rows, lon_count, channels), BF16),
            jax.ShapeDtypeStruct((2, 2, part_rows, lon_count // 2, channels), BF16),
        ],
        input_output_aliases=aliases,
        cost_estimate=pl.CostEstimate(
            flops=2 * columns * (first.size + middle.size + last.size + 256 * channels),
            bytes_accessed=8 * columns * channels,
            transcendentals=2 * columns * hidden,
        ),
    )(*operands)


def swap(value, bit):
    groups = lax.axis_size("grp")
    return lax.ppermute(value, "grp", [(g, g ^ bit) for g in range(groups)])


def join(a, b, count):
    a, b = a.astype(F32), b.astype(F32)
    total = a[0] + b[0]
    spread = (a[1] + b[1]) + jnp.square(a[0] - b[0]) * (0.5 / count)
    return jnp.stack([total, spread])


def pair_moments(stats, members):
    core = lax.axis_index("grp") % 2
    own = lax.dynamic_index_in_dim(stats, core, 0, keepdims=False)
    other = lax.dynamic_index_in_dim(stats, 1 - core, 0, keepdims=False)
    return join(own, swap(other, 1), members).astype(BF16)


def ensemble_moments(held, members):
    groups = lax.axis_size("grp")
    core = lax.axis_index("grp") % 2
    bit, count = 2, 2 * members
    while bit < groups:
        held = join(held.astype(BF16), swap(held.astype(BF16), bit), count)
        bit, count = 2 * bit, 2 * count
    scale = jnp.array([1.0 / count, 1.0 / (count - 1)], F32)
    held = (held * scale[:, None, None, None]).astype(BF16)
    partner = swap(held, 1)
    low = jnp.where(core == 0, held, partner)
    high = jnp.where(core == 0, partner, held)
    return low, high


def per_device(
    grid_state,
    noise_field,
    legendre,
    diffusion,
    input_weight,
    noise_weight,
    input_bias,
    middle_weight,
    output_weight,
):
    members, lat_rows, lon_count, channels = grid_state.shape
    wave_count = legendre.shape[1]
    bands = lax.axis_size("lat")
    local_waves = wave_count // bands
    chunk = 2
    parts = 2
    transform = wave_table(lon_count, wave_count)
    table = (
        transform.reshape(lon_count, 2, bands, local_waves)
        .transpose(0, 2, 1, 3)
        .reshape(lon_count, 2 * wave_count)
    )
    table_t = table.T
    exchange = lambda v: lax.all_to_all(v, "lat", split_axis=0, concat_axis=0, tiled=True)
    damping = damping_filter(diffusion, wave_count)

    sent = [
        analyse(grid_state, table_t, b, chunk, bands) for b in range(0, members, chunk)
    ]
    groups = lax.axis_size("grp")
    turned = legendre.transpose(1, 0, 2).reshape(bands, local_waves * lat_rows, wave_count)
    share = local_waves * lat_rows // groups
    own = lax.dynamic_slice_in_dim(turned, lax.axis_index("grp") * share, share, axis=1)
    basis = lax.all_gather(exchange(own), "grp", axis=1, tiled=True)
    basis = basis.reshape(bands, local_waves, lat_rows, wave_count).transpose(1, 0, 2, 3)
    basis = basis.reshape(local_waves, bands * lat_rows, wave_count)
    zonal_ids = lax.axis_index("lat") * local_waves + jnp.arange(local_waves, dtype=jnp.int32)
    total_ids = jnp.arange(wave_count, dtype=jnp.int32)
    triangle = total_ids[None, :] >= zonal_ids[:, None]
    basis = jnp.where(triangle[:, None], basis, jnp.zeros_like(basis))
    flipped = basis.transpose(0, 2, 1)
    received = [exchange(s) for s in sent]
    banded = [spectral(r, basis, flipped, damping, parts) for r in received]

    first = jnp.concatenate([input_weight, noise_weight], axis=0)
    new_state = None
    moments = []
    for q in range(parts):
        fields = [exchange(g[q]) for g in banded]
        if moments:
            fields, moments[-1] = lax.optimization_barrier((fields, moments[-1]))
        new_state, stats = physics(
            fields, noise_field, table, first, input_bias[None], middle_weight,
            output_weight, q, new_state,
        )
        moments.append(ensemble_moments(pair_moments(stats, members), members))
    joined = [jnp.concatenate([low, high], axis=2) for low, high in moments]
    ens_mean = jnp.concatenate([j[0] for j in joined], axis=0).astype(F32)
    ens_var = jnp.concatenate([j[1] for j in joined], axis=0).astype(F32)
    return (new_state, ens_mean, ens_var)


def solution(mesh):
    in_specs = (
        P("grp", "lat", None, None),
        P("grp", "lat", None, None),
        P("lat", None, None),
        P(),
        P(),
        P(),
        P(),
        P(),
        P(),
    )
    out_specs = (P("grp", "lat", None, None), P("lat", None, None), P("lat", None, None))
    return jax.shard_map(
        per_device, mesh=mesh, in_specs=in_specs, out_specs=out_specs, check_vma=False
    )
```
